512 devices in a mesh: node: 32 (over y, x, core), freq: 16 (over z).
Axes of the slice: x: 4, y: 4, z: 16, core: 2. Of those that a mesh axis runs over, the one named last changes fastest.
Arguments:
- density: float32 [256, 16, 8192], P('freq', None, 'node'), may hold values from -6 to 6
- coords: float32 [3, 8192], P(None, 'node'), may hold values from -12 to 12
- weights: float32 [8192], P('node'), may hold values from 0.1 to 1
- neighbours: int32 [64, 4], P('node'), may hold values from 0 to 63, as said below
- counts: int32 [64], P('node'), may hold values from 1 to 4, as said below
Outputs:
- field: float32 [256, 16, 8192], P('freq', None, 'node')
The draws below stay inside these ranges and needn't reach their ends.
Inputs may be any that keep to these rules, and one draw needn't show every extreme that they name: `neighbours`: row p starts with p itself, then lists distinct patches that lie within 2 places of p in the cyclic order of patches; only the first counts[p] entries of a row are used, the rest are valid patch numbers. `counts`: some patch uses all 4 entries.
All inputs are finite; a program needn't handle non-finite values.
Results may differ from the reference program's by a relative error of at most 0.0003.
Values sent between devices are 32-bit elements; how exact they have to be, the bound alone decides.
A program may use at most 64 MiB of HBM per device.

```python
import math
import jax
import jax.numpy as jnp
from jax import lax

STEPS = 256
FIELDS = 16
PATCH = 128
PATCH_DEV = 2
NEAR_MOST = 4
PATCHES = 64
NODES = 8192


def adjacency_helper(key):
    base_key = jax.random.fold_in(key, 7)
    count_key, force_key, order_key = jax.random.split(base_key, 3)
    live_counts = jax.random.randint(count_key, (PATCHES,), 1, NEAR_MOST + 1)
    chosen = jax.random.randint(force_key, (), 0, PATCHES)
    live_counts = jnp.where(jnp.arange(PATCHES) == chosen, NEAR_MOST, live_counts)
    span_size = 2 * PATCH_DEV
    scores = jax.random.randint(order_key, (PATCHES, span_size), 0, 1 << 20) * span_size + jnp.arange(span_size)[None, :]
    ordering = jnp.argsort(scores, axis=1)
    offsets = jnp.where(ordering < PATCH_DEV, ordering - PATCH_DEV, ordering - PATCH_DEV + 1)
    picked = offsets[:, :NEAR_MOST - 1]
    own_patch = jnp.arange(PATCHES)[:, None]
    listing = jnp.concatenate([own_patch, (own_patch + picked) % PATCHES], axis=1)
    return (listing.astype(jnp.int32), live_counts.astype(jnp.int32))


def draw_neighbours(key, part):
    listing, live_counts = adjacency_helper(key)
    return listing


def draw_counts(key, part):
    listing, live_counts = adjacency_helper(key)
    return live_counts


def draw_coords(key, part):
    jitter_key = jax.random.fold_in(key, 11)
    patch_ids = (jnp.arange(NODES) // PATCH).astype(jnp.float32)
    phase_angle = 2.0 * jnp.pi * patch_ids / PATCHES
    radius = PATCHES / (2.0 * jnp.pi)
    centres = jnp.stack([radius * jnp.cos(phase_angle), radius * jnp.sin(phase_angle), jnp.zeros_like(phase_angle)])
    jitter = jax.random.uniform(jitter_key, (3, NODES), jnp.float32, -0.5, 0.5)
    return (centres + jitter).astype(jnp.float32)


def levels(rng, shape, pieces, low, top_value):
    factor_of = 1.0
    for position, blocks in pieces:
        draws = jax.random.uniform(jax.random.fold_in(jax.random.fold_in(rng, 6), position), (blocks,), jnp.float32, low / len(pieces), top_value / len(pieces))
        factor_of = factor_of * jnp.repeat(jnp.exp(draws), shape[position] // blocks).reshape((-1,) + (1,) * (len(shape) - 1 - position))
    return factor_of


def bell_draw(key, extent, spread, bound, cuts=(), kind=jnp.bfloat16):
    array = spread * jax.random.normal(key, extent, jnp.float32)
    if cuts:
        array = array * levels(key, extent, cuts, -0.22, 0.18)
    return jnp.clip(array, -bound, bound).astype(kind)


def setup_inputs(seed: int = 0) -> dict:
    key_of = jax.random.split(jax.random.key(seed), 6)
    density = bell_draw(key_of[0], (STEPS, FIELDS, NODES), 1.0, 6.0, ((0, 16), (2, 32)), jnp.float32)
    coords = draw_coords(jax.random.fold_in(key_of[5], 71), 0)
    weights = jnp.clip(jnp.exp(math.log(1.0) - 2.3025851 * jax.random.uniform(key_of[2], (NODES,), jnp.float32) ** levels(key_of[2], (NODES,), ((0, 32),), -0.2, 0.2)), 0.1, 1.0)
    neighbours = draw_neighbours(jax.random.fold_in(key_of[5], 71), 0)
    counts = draw_counts(jax.random.fold_in(key_of[5], 71), 0)
    return dict(density=density, coords=coords, weights=weights, neighbours=neighbours, counts=counts)


decay_ratio = 0.1
time_step = 1.0
smoothing = 0.5
highest = lax.Precision.HIGHEST

def fourier_tables(freq_count):
    freq_index = jnp.arange(freq_count, dtype=jnp.int32)
    time_index = jnp.arange(STEPS, dtype=jnp.int32)
    phase_index = (2 * freq_index[:, None] + 1) * time_index[None, :] % (2 * STEPS)
    phase_angle = phase_index.astype(jnp.float32) * (jnp.pi / STEPS)
    return (jnp.cos(phase_angle), jnp.sin(phase_angle))

def laplace_values(freq_index):
    phase_angle = (2 * freq_index + 1).astype(jnp.float32) * (jnp.pi / STEPS)
    radius = decay_ratio ** (1.0 / STEPS)
    offset_real = 1.0 - radius * jnp.cos(phase_angle)
    offset_imag = -radius * jnp.sin(phase_angle)
    delta_real = offset_real + 0.5 * (offset_real * offset_real - offset_imag * offset_imag)
    delta_imag = offset_imag + offset_real * offset_imag
    return (delta_real / time_step, delta_imag / time_step)

def time_weights(time_index, sign):
    radius = decay_ratio ** (1.0 / STEPS)
    return jnp.power(jnp.float32(radius), sign * time_index.astype(jnp.float32))

def kernel_terms(distance, static_part, value_real, value_imag):
    decaying = jnp.exp(-value_real * distance) * static_part
    return (decaying * jnp.cos(value_imag * distance), -decaying * jnp.sin(value_imag * distance))

def reference(density, coords, weights, neighbours, counts):
    half_count = STEPS // 2
    cosine, sine = fourier_tables(half_count)
    time_index = jnp.arange(STEPS, dtype=jnp.int32)
    scaled = density * time_weights(time_index, 1.0)[:, None, None]
    flattened = scaled.reshape(STEPS, FIELDS * NODES)
    spec_real = jnp.dot(cosine, flattened, precision=highest, preferred_element_type=jnp.float32).reshape(half_count, FIELDS, NODES)
    spec_imag = jnp.dot(sine, flattened, precision=highest, preferred_element_type=jnp.float32).reshape(half_count, FIELDS, NODES)
    laplace_real, laplace_imag = laplace_values(jnp.arange(half_count, dtype=jnp.int32))
    slot_index = jnp.arange(NEAR_MOST, dtype=jnp.int32)
    node_offset = jnp.arange(PATCH, dtype=jnp.int32)

    def one_patch(patch_index):
        own_coords = lax.dynamic_slice_in_dim(coords, patch_index * PATCH, PATCH, 1)
        columns = (neighbours[patch_index][:, None] * PATCH + node_offset[None, :]).reshape(NEAR_MOST * PATCH)
        other_coords = coords[:, columns]
        live_slots = (slot_index < counts[patch_index]).astype(jnp.float32)
        node_scale = weights[columns] * jnp.repeat(live_slots, PATCH)
        separation = own_coords[:, :, None] - other_coords[:, None, :]
        distance = jnp.sqrt(lax.optimization_barrier(jnp.sum(separation * separation, axis=0)) + smoothing * smoothing)
        static_part = node_scale[None, :] / (4.0 * jnp.pi * distance)
        near_real = spec_real[:, :, columns]
        near_imag = spec_imag[:, :, columns]
        kern_real, kern_imag = kernel_terms(distance[None], static_part[None], laplace_real[:, None, None], laplace_imag[:, None, None])
        out_real = jnp.einsum('fij,frj->fri', kern_real, near_real, precision=highest) - jnp.einsum('fij,frj->fri', kern_imag, near_imag, precision=highest)
        out_imag = jnp.einsum('fij,frj->fri', kern_real, near_imag, precision=highest) + jnp.einsum('fij,frj->fri', kern_imag, near_real, precision=highest)
        return (out_real, out_imag)
    result_real, result_imag = lax.map(one_patch, jnp.arange(PATCHES, dtype=jnp.int32))
    result_real = jnp.transpose(result_real, (1, 2, 0, 3)).reshape(half_count, FIELDS * NODES)
    result_imag = jnp.transpose(result_imag, (1, 2, 0, 3)).reshape(half_count, FIELDS * NODES)
    summed = jnp.dot(cosine.T, result_real, precision=highest, preferred_element_type=jnp.float32) + jnp.dot(sine.T, result_imag, precision=highest, preferred_element_type=jnp.float32)
    summed = summed * (2.0 / STEPS) * time_weights(time_index, -1.0)[:, None]
    return summed.reshape(STEPS, FIELDS, NODES)
```

```python
import functools

import jax
import jax.numpy as jnp
import ml_dtypes
import numpy as np
from jax import lax
from jax.experimental import pallas as pl
from jax.experimental.pallas import tpu as pltpu
from jax.sharding import PartitionSpec as P

MESH = pl.DeviceIdType.MESH
PATCH = 128
PATCH_DEV = 2
NEAR_MOST = 4
WIDTH = PATCH * PATCH_DEV
DECAY = 0.1
SMOOTH = 0.25
GEN_ROWS = 64


def split_bf16(table):
    high = table.astype(np.float32).astype(ml_dtypes.bfloat16)
    low = (table - high.astype(np.float64)).astype(np.float32).astype(ml_dtypes.bfloat16)
    return high, low


def transform_tables(steps):
    freq = np.arange(steps // 2)[:, None, None]
    part = np.arange(2)[None, :, None]
    time = np.arange(steps)[None, None, :]
    angle = ((2 * freq + 1) * time % (2 * steps)) * (np.pi / steps)
    waves = np.where(part == 0, np.cos(angle), np.sin(angle)).reshape(steps, steps)
    growth = DECAY ** (np.arange(steps) / steps)
    forward = waves * growth[None, :]
    inverse = waves.T * (2.0 / steps / growth)[:, None]
    return np.concatenate(split_bf16(forward) + split_bf16(inverse), axis=0)


def laplace_table(steps):
    angle = (2 * np.arange(steps // 2) + 1) * (np.pi / steps)
    zeta = DECAY ** (1.0 / steps) * np.exp(1j * angle)
    delta = (1 - zeta) + (1 - zeta) ** 2 / 2
    return np.stack([-delta.real * np.log2(np.e), delta.imag / (2 * np.pi)]).astype(np.float32)


def fit_even(function, degree):
    nodes = 0.125 + 0.125 * np.cos(np.pi * (np.arange(200) + 0.5) / 200)
    fitted = np.polynomial.chebyshev.Chebyshev.fit(nodes, function(np.sqrt(nodes)), degree, domain=[0, 0.25])
    return [float(c) for c in fitted.convert(kind=np.polynomial.Polynomial).coef]


SINE = fit_even(lambda f: np.sin(np.pi * f) / f, 4)
COSINE = fit_even(lambda f: np.cos(np.pi * f), 4)


def horner(coefficients, value):
    total = coefficients[-1] * value + coefficients[-2]
    for coefficient in coefficients[-3::-1]:
        total = total * value + coefficient
    return total


def halves(value):
    high = value.astype(jnp.bfloat16)
    return high, (value - high.astype(jnp.float32)).astype(jnp.bfloat16)


def dot(left, right):
    return jnp.dot(left, right, preferred_element_type=jnp.float32)


def kernel(
    parts,
    node_parts,
    x_hbm,
    table_hbm,
    coords_ref,
    weights_ref,
    near_ref,
    counts_ref,
    laplace_ref,
    out_hbm,
    x_vmem,
    table,
    send1,
    recv1,
    send2,
    halo,
    picked,
    send3,
    recv3,
    send4,
    recv4,
    out_vmem,
    places,
    distance,
    static,
    kern_high,
    kern_low,
    local_sem,
    send_sem,
    recv_sem,
    halo_send,
    halo_recv,
    place_send,
    place_recv,
):
    me = lax.axis_index("freq")
    node = lax.axis_index("node")
    steps = parts * 16
    fields = parts
    right = lax.rem(node + 1, node_parts)
    left = lax.rem(node + node_parts - 1, node_parts)
    order = sorted(range(1, parts), key=lambda k: -min(k, parts - k))
    peers = [lax.rem(me + k, parts) for k in order]
    mine = pl.ds(pl.multiple_of(me * 16, 16), 16)

    loads = [
        pltpu.make_async_copy(x_hbm.at[:, pl.ds(p * PATCH, PATCH)], x_vmem.at[p], local_sem.at[p])
        for p in range(PATCH_DEV)
    ]
    loads.append(pltpu.make_async_copy(table_hbm, table, local_sem.at[2]))
    for load in loads:
        load.start()
    barrier = pltpu.get_barrier_semaphore()
    for peer in peers:
        pl.semaphore_signal(barrier, inc=1, device_id={"freq": peer}, device_id_type=MESH)
    for side in (left, right):
        pl.semaphore_signal(barrier, inc=1, device_id={"node": side}, device_id_type=MESH)

    for p in range(PATCH_DEV):
        span = pl.ds(p * PATCH, PATCH)
        places[2 + p, 0:3, :] = coords_ref[:, span]
        places[2 + p, 3:4, :] = weights_ref[:, span]
        places[2 + p, 4:8, :] = jnp.zeros((4, PATCH), jnp.float32)
    for p in range(PATCH_DEV):
        loads[p].wait()
        for f in range(fields):
            send1[p, pl.ds(f * 16, 16), :] = x_vmem[p, pl.ds(f, 16, stride=fields), :]
        recv1[p, mine, :] = send1[p, mine, :]
    pl.semaphore_wait(barrier, parts + 1)

    def exchange(phase, p, source, target):
        for peer in peers:
            pltpu.make_async_remote_copy(
                src_ref=source.at[pl.ds(pl.multiple_of(peer * 16, 16), 16)],
                dst_ref=target.at[mine],
                send_sem=send_sem.at[phase, p],
                recv_sem=recv_sem.at[phase, p],
                device_id={"freq": peer},
                device_id_type=MESH,
            ).start()

    def whole(phase, p, source, target):
        rows = pl.ds(0, (parts - 1) * 16)
        return pltpu.make_async_remote_copy(
            src_ref=source.at[rows],
            dst_ref=target.at[rows],
            send_sem=send_sem.at[phase, p],
            recv_sem=recv_sem.at[phase, p],
            device_id={"freq": peers[0]},
            device_id_type=MESH,
        )

    place_copies = [
        pltpu.make_async_remote_copy(
            src_ref=places.at[pl.ds(2, 2)],
            dst_ref=places.at[pl.ds(slot, 2)],
            send_sem=place_send.at[slot // 4],
            recv_sem=place_recv.at[slot // 4],
            device_id={"node": side},
            device_id_type=MESH,
        )
        for side, slot in ((right, 0), (left, 4))
    ]
    for copy in place_copies:
        copy.start()
    for p in range(PATCH_DEV):
        exchange(0, p, send1.at[p], recv1.at[p])

    for copy in place_copies:
        copy.wait_recv()
    total_patches = PATCH_DEV * node_parts

    def slot_of(p, k):
        slot = lax.rem(near_ref[p, k] - (node - 1) * PATCH_DEV + total_patches, total_patches)
        return jnp.clip(slot, 0, 3 * PATCH_DEV - 1)

    slots = [[slot_of(p, k) for k in range(NEAR_MOST)] for p in range(PATCH_DEV)]
    for p in range(PATCH_DEV):
        for k in range(NEAR_MOST):
            column = places[slots[p][k]].T
            total = SMOOTH
            for c in range(3):
                apart = column[:, c : c + 1] - coords_ref[c : c + 1, p * PATCH : (p + 1) * PATCH]
                total = total + apart * apart
            inverse = lax.rsqrt(total)
            live = jnp.where(k < counts_ref[p], 1.0 / (4.0 * np.pi), 0.0)
            rows = pl.ds((p * NEAR_MOST + k) * PATCH, PATCH)
            distance[rows, :] = total * inverse
            static[rows, :] = (column[:, 3:4] * live) * inverse

    blocks = PATCH_DEV * NEAR_MOST * PATCH // GEN_ROWS

    def generate(step, carry):
        l = step // blocks
        block = step % blocks
        rows = pl.ds(pl.multiple_of(block * GEN_ROWS, GEN_ROWS), GEN_ROWS)
        radius = distance[rows, :]
        decaying = jnp.exp2(radius * laplace_ref[0, me * 8 + l]) * static[rows, :]
        turns = radius * laplace_ref[1, me * 8 + l]
        turns = turns - jnp.round(turns)
        square = turns * turns
        sine = horner(SINE, square) * turns
        cosine = horner([-c for c in COSINE], square)
        double = decaying * sine
        double = double + double
        real_high, real_low = halves(decaying - double * sine)
        imag_high, imag_low = halves(double * cosine)
        into = pl.ds(pl.multiple_of(step * GEN_ROWS, GEN_ROWS), GEN_ROWS)
        kern_high[into, 0:PATCH] = real_high
        kern_high[into, PATCH : 2 * PATCH] = imag_high
        kern_low[into, 0:PATCH] = real_low
        kern_low[into, PATCH : 2 * PATCH] = imag_low
        return carry

    lax.fori_loop(0, 8 * blocks, generate, 0)

    def transform(index, data):
        data_high, data_low = halves(data)
        table_high = table[pl.ds(2 * index * steps, steps), :]
        table_low = table[pl.ds((2 * index + 1) * steps, steps), :]
        first = dot(table_high, jnp.concatenate([data_high, data_low], axis=1))
        return first[:, :PATCH] + first[:, PATCH:] + dot(table_low, data_high)

    loads[2].wait()
    for p in range(PATCH_DEV):
        whole(0, p, send1.at[p], recv1.at[p]).wait_recv()
        send2[p] = transform(0, recv1[p])
        halo[2 + p, mine, :] = send2[p, mine, :]
        exchange(1, p, send2.at[p], halo.at[2 + p])

    halo_copies = []
    for p in range(PATCH_DEV):
        whole(1, p, send2.at[p], halo.at[2 + p]).wait_recv()
        for side, slot in ((right, 0), (left, 4)):
            copy = pltpu.make_async_remote_copy(
                src_ref=halo.at[2 + p],
                dst_ref=halo.at[slot + p],
                send_sem=halo_send.at[slot // 4, p],
                recv_sem=halo_recv.at[slot // 4, p],
                device_id={"node": side},
                device_id_type=MESH,
            )
            copy.start()
            halo_copies.append(copy)
    for copy in halo_copies:
        copy.wait_recv()

    for p in range(PATCH_DEV):
        for k in range(NEAR_MOST):
            picked[p * NEAR_MOST + k] = halo[slots[p][k]]
        for l in range(8):
            both = jnp.concatenate(
                [
                    jnp.concatenate(
                        [picked[p * NEAR_MOST + k, pl.ds(2 * l + ri, fields, stride=16), :] for k in range(NEAR_MOST)],
                        axis=1,
                    )
                    for ri in range(2)
                ],
                axis=0,
            )
            both_high, both_low = halves(both)
            rows = pl.ds((l * PATCH_DEV + p) * NEAR_MOST * PATCH, NEAR_MOST * PATCH)
            first = dot(jnp.concatenate([both_high, both_low], axis=0), kern_high[rows, :])
            total = first[: 2 * fields] + first[2 * fields :] + dot(both_high, kern_low[rows, :])
            send3[p, pl.ds(2 * l, fields, stride=16), :] = total[:fields, :PATCH] - total[fields:, PATCH:]
            send3[p, pl.ds(2 * l + 1, fields, stride=16), :] = total[fields:, :PATCH] + total[:fields, PATCH:]
        recv3[p, mine, :] = send3[p, mine, :]
        exchange(2, p, send3.at[p], recv3.at[p])

    for p in range(PATCH_DEV):
        whole(2, p, send3.at[p], recv3.at[p]).wait_recv()
        send4[p] = transform(1, recv3[p])
        recv4[p, mine, :] = send4[p, mine, :]
        exchange(3, p, send4.at[p], recv4.at[p])

    stores = []
    for p in range(PATCH_DEV):
        whole(3, p, send4.at[p], recv4.at[p]).wait_recv()
        for f in range(fields):
            out_vmem[p, pl.ds(f, 16, stride=fields), :] = recv4[p, pl.ds(f * 16, 16), :]
        store = pltpu.make_async_copy(out_vmem.at[p], out_hbm.at[:, pl.ds(p * PATCH, PATCH)], local_sem.at[p])
        store.start()
        stores.append(store)

    for copy in place_copies + halo_copies:
        copy.wait_send()
    for p in range(PATCH_DEV):
        whole(0, p, send1.at[p], recv1.at[p]).wait_send()
        whole(1, p, send2.at[p], halo.at[2 + p]).wait_send()
        whole(2, p, send3.at[p], recv3.at[p]).wait_send()
        whole(3, p, send4.at[p], recv4.at[p]).wait_send()
    for store in stores:
        store.wait()


def body(density, coords, weights, neighbours, counts):
    parts = lax.axis_size("freq")
    node_parts = lax.axis_size("node")
    times, fields, width = density.shape
    steps = times * parts
    assert times == 16 and fields == parts and width == WIDTH
    rows = times * fields
    vmem = pl.BlockSpec(memory_space=pltpu.VMEM)
    smem = pl.BlockSpec(memory_space=pltpu.SMEM)
    hbm = pl.BlockSpec(memory_space=pltpu.HBM)
    buffer = pltpu.VMEM((PATCH_DEV, steps, PATCH), jnp.float32)
    pairs = PATCH_DEV * NEAR_MOST * PATCH
    result = pl.pallas_call(
        functools.partial(kernel, parts, node_parts),
        out_shape=jax.ShapeDtypeStruct((rows, width), jnp.float32),
        in_specs=[hbm, hbm, vmem, vmem, smem, smem, smem],
        out_specs=pl.BlockSpec(memory_space=pl.ANY),
        scratch_shapes=[
            pltpu.VMEM((PATCH_DEV, rows, PATCH), jnp.float32),
            pltpu.VMEM((4 * steps, steps), jnp.bfloat16),
            buffer,
            buffer,
            buffer,
            pltpu.VMEM((3 * PATCH_DEV, steps, PATCH), jnp.float32),
            pltpu.VMEM((PATCH_DEV * NEAR_MOST, steps, PATCH), jnp.float32),
            buffer,
            buffer,
            buffer,
            buffer,
            pltpu.VMEM((PATCH_DEV, rows, PATCH), jnp.float32),
            pltpu.VMEM((3 * PATCH_DEV, 8, PATCH), jnp.float32),
            pltpu.VMEM((pairs, PATCH), jnp.float32),
            pltpu.VMEM((pairs, PATCH), jnp.float32),
            pltpu.VMEM((8 * pairs, 2 * PATCH), jnp.bfloat16),
            pltpu.VMEM((8 * pairs, 2 * PATCH), jnp.bfloat16),
            pltpu.SemaphoreType.DMA((3,)),
            pltpu.SemaphoreType.DMA((4, PATCH_DEV)),
            pltpu.SemaphoreType.DMA((4, PATCH_DEV)),
            pltpu.SemaphoreType.DMA((2, PATCH_DEV)),
            pltpu.SemaphoreType.DMA((2, PATCH_DEV)),
            pltpu.SemaphoreType.DMA((2,)),
            pltpu.SemaphoreType.DMA((2,)),
        ],
        compiler_params=pltpu.CompilerParams(
            collective_id=0, has_side_effects=True, vmem_limit_bytes=60_000_000
        ),
    )(
        density.reshape(rows, width),
        jnp.asarray(transform_tables(steps)),
        coords,
        weights.reshape(1, width),
        neighbours,
        counts,
        jnp.asarray(laplace_table(steps)),
    )
    return result.reshape(times, fields, width)


def solution(mesh):
    placed = (P("freq", None, "node"), P(None, "node"), P("node"), P("node", None), P("node"))
    return jax.shard_map(
        body, mesh=mesh, in_specs=placed, out_specs=P("freq", None, "node"), check_vma=False
    )
```

```python
import functools

import jax
import jax.numpy as jnp
import ml_dtypes
import numpy as np
from jax import lax
from jax.experimental import pallas as pl
from jax.experimental.pallas import tpu as pltpu
from jax.sharding import PartitionSpec as P

MESH = pl.DeviceIdType.MESH
PATCH = 128
PATCH_DEV = 2
NEAR_MOST = 4
WIDTH = PATCH * PATCH_DEV
DECAY = 0.1
SMOOTH = 0.25
GEN_ROWS = 64


def split_bf16(table):
    high = table.astype(np.float32).astype(ml_dtypes.bfloat16)
    low = (table - high.astype(np.float64)).astype(np.float32).astype(ml_dtypes.bfloat16)
    return high, low


def transform_tables(steps):
    freq = np.arange(steps // 2)[:, None, None]
    part = np.arange(2)[None, :, None]
    time = np.arange(steps)[None, None, :]
    angle = ((2 * freq + 1) * time % (2 * steps)) * (np.pi / steps)
    waves = np.where(part == 0, np.cos(angle), np.sin(angle)).reshape(steps, steps)
    waves = waves.reshape(steps // 16, 2, 8, steps).transpose(1, 0, 2, 3).reshape(steps, steps)
    growth = DECAY ** (np.arange(steps) / steps)
    forward = waves * growth[None, :]
    inverse = waves.T * (2.0 / steps / growth)[:, None]
    return np.concatenate(split_bf16(forward) + split_bf16(inverse), axis=0)


def laplace_table(steps):
    angle = (2 * np.arange(steps // 2) + 1) * (np.pi / steps)
    zeta = DECAY ** (1.0 / steps) * np.exp(1j * angle)
    delta = (1 - zeta) + (1 - zeta) ** 2 / 2
    return np.stack([-delta.real * np.log2(np.e), delta.imag / (2 * np.pi)]).astype(np.float32)


def fit_even(function, degree):
    nodes = 0.125 + 0.125 * np.cos(np.pi * (np.arange(200) + 0.5) / 200)
    fitted = np.polynomial.chebyshev.Chebyshev.fit(nodes, function(np.sqrt(nodes)), degree, domain=[0, 0.25])
    return [float(c) for c in fitted.convert(kind=np.polynomial.Polynomial).coef]


SINE = fit_even(lambda f: np.sin(np.pi * f) / f, 4)
COSINE = fit_even(lambda f: np.cos(np.pi * f), 4)


def horner(coefficients, value):
    total = coefficients[-1] * value + coefficients[-2]
    for coefficient in coefficients[-3::-1]:
        total = total * value + coefficient
    return total


def halves(value):
    high = value.astype(jnp.bfloat16)
    return high, (value - high.astype(jnp.float32)).astype(jnp.bfloat16)


def dot(left, right):
    return jnp.dot(left, right, preferred_element_type=jnp.float32)


def kernel(
    parts,
    node_parts,
    x_hbm,
    table_hbm,
    coords_hbm,
    weights_hbm,
    near_hbm,
    counts_hbm,
    laplace_hbm,
    out_ref,
    x_vmem,
    table,
    coords_ref,
    weights_ref,
    near_ref,
    counts_ref,
    laplace_ref,
    send1,
    recv1,
    send2,
    halo_first,
    halo_second,
    picked,
    send3,
    recv3,
    send4,
    recv4,
    places,
    distance,
    static,
    kern_high,
    kern_low,
    local_sem,
    chain_sem,
    send_sem,
    recv_sem,
    half_send,
    half_recv,
    halo_send,
    halo_recv,
    place_send,
    place_recv,
):
    halo = (halo_first, halo_second)
    me = lax.axis_index("freq")
    node = lax.axis_index("node")
    steps = parts * 16
    fields = parts
    reach = parts // 4
    right = lax.rem(node + 1, node_parts)
    left = lax.rem(node + node_parts - 1, node_parts)

    def peers_of(order):
        return [lax.rem(me + k, parts) for k in order]

    def by_hops(first, last):
        order = [k for k in range(1, parts) if first <= min(k, parts - k) <= last]
        return peers_of(sorted(order, key=lambda k: -min(k, parts - k)))

    near_peers = by_hops(1, reach)
    far_peers = by_hops(reach + 1, 2 * reach)
    peers = far_peers + near_peers
    chain_peers = peers_of((reach, parts - reach))

    loads = [
        pltpu.make_async_copy(x_hbm.at[:, pl.ds(p * PATCH, PATCH)], x_vmem.at[p], local_sem.at[p])
        for p in range(PATCH_DEV)
    ]
    for source, target in (
        (coords_hbm, coords_ref),
        (weights_hbm, weights_ref),
        (near_hbm, near_ref),
        (counts_hbm, counts_ref),
        (laplace_hbm, laplace_ref),
        (table_hbm, table),
    ):
        loads.append(pltpu.make_async_copy(source, target, local_sem.at[len(loads)]))
    for load in loads:
        load.start()
    barrier = pltpu.get_barrier_semaphore()
    for peer in near_peers:
        pl.semaphore_signal(barrier, inc=1, device_id={"freq": peer}, device_id_type=MESH)
    for side in (left, right):
        pl.semaphore_signal(barrier, inc=1, device_id={"node": side}, device_id_type=MESH)

    def block(index, rows):
        return pl.ds(pl.multiple_of(index * rows, rows), rows)

    mine = block(me, 16)
    for p in range(PATCH_DEV):
        loads[p].wait()
        for f in range(fields):
            send1[p, pl.ds(f * 16, 16), :] = x_vmem[p, pl.ds(f, 16, stride=fields), :]
        recv1[p, mine, :] = send1[p, mine, :]
    for load in loads[2:7]:
        load.wait()
    for p in range(PATCH_DEV):
        span = pl.ds(p * PATCH, PATCH)
        places[2 + p, 0:3, :] = coords_ref[:, span]
        places[2 + p, 3:4, :] = weights_ref[:, span]
        places[2 + p, 4:8, :] = jnp.zeros((4, PATCH), jnp.float32)
    pl.semaphore_wait(barrier, len(near_peers) + 2)

    def push(peer, source, target, rows, sends, receives):
        pltpu.make_async_remote_copy(
            src_ref=source.at[block(peer, rows)],
            dst_ref=target.at[block(me, rows)],
            send_sem=sends,
            recv_sem=receives,
            device_id={"freq": peer},
            device_id_type=MESH,
        ).start()

    def whole(source, target, rows, sends, receives):
        span = pl.ds(0, (parts - 1) * rows)
        return pltpu.make_async_remote_copy(
            src_ref=source.at[span],
            dst_ref=target.at[span],
            send_sem=sends,
            recv_sem=receives,
            device_id={"freq": peers[0]},
            device_id_type=MESH,
        )

    def full(phase, p):
        source, target = ((send1, recv1), (send4, recv4))[phase]
        return source.at[p], target.at[p], 16, send_sem.at[phase, p], recv_sem.at[phase, p]

    def part(phase, p, h):
        source, target = ((send2.at[p, h], halo[h].at[2 + p]), (send3.at[p, h], recv3.at[p, h]))[phase]
        return source, target, 8, half_send.at[phase, p, h], half_recv.at[phase, p, h]

    for peer in chain_peers:
        pl.semaphore_signal(chain_sem, inc=1, device_id={"freq": peer}, device_id_type=MESH)
    place_copies = [
        pltpu.make_async_remote_copy(
            src_ref=places.at[pl.ds(2, 2)],
            dst_ref=places.at[pl.ds(slot, 2)],
            send_sem=place_send.at[slot // 4],
            recv_sem=place_recv.at[slot // 4],
            device_id={"node": side},
            device_id_type=MESH,
        )
        for side, slot in ((right, 0), (left, 4))
    ]
    for copy in place_copies:
        copy.start()
    for p in range(PATCH_DEV):
        for peer in near_peers:
            push(peer, *full(0, p))
    pl.semaphore_wait(chain_sem, 2)
    for p in range(PATCH_DEV):
        for peer in far_peers:
            push(peer, *full(0, p))

    for copy in place_copies:
        copy.wait_recv()
    total_patches = PATCH_DEV * node_parts

    def slot_of(p, k):
        slot = lax.rem(near_ref[p, k] - (node - 1) * PATCH_DEV + total_patches, total_patches)
        return jnp.clip(slot, 0, 3 * PATCH_DEV - 1)

    slots = [[slot_of(p, k) for k in range(NEAR_MOST)] for p in range(PATCH_DEV)]
    for p in range(PATCH_DEV):
        for k in range(NEAR_MOST):
            column = places[slots[p][k]].T
            total = SMOOTH
            for c in range(3):
                apart = column[:, c : c + 1] - coords_ref[c : c + 1, p * PATCH : (p + 1) * PATCH]
                total = total + apart * apart
            inverse = lax.rsqrt(total)
            live = jnp.where(k < counts_ref[p], 1.0 / (4.0 * np.pi), 0.0)
            rows = pl.ds((p * NEAR_MOST + k) * PATCH, PATCH)
            distance[rows, :] = total * inverse
            static[rows, :] = (column[:, 3:4] * live) * inverse

    blocks = PATCH_DEV * NEAR_MOST * PATCH // GEN_ROWS

    def generate(step, carry):
        l = step // blocks
        rows = block(step % blocks, GEN_ROWS)
        radius = distance[rows, :]
        decaying = jnp.exp2(radius * laplace_ref[0, me * 8 + l]) * static[rows, :]
        turns = radius * laplace_ref[1, me * 8 + l]
        turns = turns - jnp.round(turns)
        square = turns * turns
        sine = horner(SINE, square) * turns
        cosine = horner([-c for c in COSINE], square)
        double = decaying * sine
        double = double + double
        real_high, real_low = halves(decaying - double * sine)
        imag_high, imag_low = halves(double * cosine)
        into = block(step, GEN_ROWS)
        kern_high[into, 0:PATCH] = real_high
        kern_high[into, PATCH : 2 * PATCH] = imag_high
        kern_low[into, 0:PATCH] = real_low
        kern_low[into, PATCH : 2 * PATCH] = imag_low
        return carry

    lax.fori_loop(0, 4 * blocks, generate, 0)

    def transform(index, data):
        data_high, data_low = halves(data)
        table_high = table[pl.ds(2 * index * steps, steps), :]
        table_low = table[pl.ds((2 * index + 1) * steps, steps), :]
        first = dot(table_high, jnp.concatenate([data_high, data_low], axis=1))
        return first[:, :PATCH] + first[:, PATCH:] + dot(table_low, data_high)

    half_rows = parts * 8
    loads[7].wait()
    for p in range(PATCH_DEV):
        whole(*full(0, p)).wait_recv()
        spectrum = transform(0, recv1[p])
        for h in range(2):
            send2[p, h] = spectrum[h * half_rows : (h + 1) * half_rows]
            halo[h][2 + p, block(me, 8), :] = send2[p, h, block(me, 8), :]
        for peer in peers:
            push(peer, *part(0, p, 0))
    for p in range(PATCH_DEV):
        for peer in peers:
            push(peer, *part(0, p, 1))

    lax.fori_loop(4 * blocks, 8 * blocks, generate, 0)

    halo_copies = {}

    def spread(p, h):
        whole(*part(0, p, h)).wait_recv()
        for side, slot in ((right, 0), (left, 4)):
            copy = pltpu.make_async_remote_copy(
                src_ref=halo[h].at[2 + p],
                dst_ref=halo[h].at[slot + p],
                send_sem=halo_send.at[slot // 4, p, h],
                recv_sem=halo_recv.at[slot // 4, p, h],
                device_id={"node": side},
                device_id_type=MESH,
            )
            copy.start()
            halo_copies[slot, p, h] = copy

    def near_field(h):
        for p in range(PATCH_DEV):
            for slot in (0, 4):
                halo_copies[slot, p, h].wait_recv()
        for p in range(PATCH_DEV):
            for k in range(NEAR_MOST):
                picked[h, p * NEAR_MOST + k] = halo[h][slots[p][k]]
            for l in range(4):
                both = jnp.concatenate(
                    [
                        jnp.concatenate(
                            [
                                picked[h, p * NEAR_MOST + k, pl.ds(2 * l + ri, fields, stride=8), :]
                                for k in range(NEAR_MOST)
                            ],
                            axis=1,
                        )
                        for ri in range(2)
                    ],
                    axis=0,
                )
                both_high, both_low = halves(both)
                start = ((4 * h + l) * PATCH_DEV + p) * NEAR_MOST * PATCH
                rows = pl.ds(start, NEAR_MOST * PATCH)
                first = dot(jnp.concatenate([both_high, both_low], axis=0), kern_high[rows, :])
                total = first[: 2 * fields] + first[2 * fields :] + dot(both_high, kern_low[rows, :])
                send3[p, h, pl.ds(2 * l, fields, stride=8), :] = total[:fields, :PATCH] - total[fields:, PATCH:]
                send3[p, h, pl.ds(2 * l + 1, fields, stride=8), :] = total[fields:, :PATCH] + total[:fields, PATCH:]
            recv3[p, h, block(me, 8), :] = send3[p, h, block(me, 8), :]
            for peer in peers:
                push(peer, *part(1, p, h))

    spread(0, 0)
    spread(1, 0)
    spread(0, 1)
    near_field(0)
    spread(1, 1)
    near_field(1)

    for p in range(PATCH_DEV):
        for h in range(2):
            whole(*part(1, p, h)).wait_recv()
        send4[p] = transform(1, jnp.concatenate([recv3[p, 0], recv3[p, 1]], axis=0))
        recv4[p, mine, :] = send4[p, mine, :]
        for peer in peers:
            push(peer, *full(1, p))

    for p in range(PATCH_DEV):
        whole(*full(1, p)).wait_recv()
        for f in range(fields):
            out_ref[p, pl.ds(f, 16, stride=fields), :] = recv4[p, pl.ds(f * 16, 16), :]

    for copy in place_copies + list(halo_copies.values()):
        copy.wait_send()
    for p in range(PATCH_DEV):
        whole(*full(0, p)).wait_send()
        whole(*full(1, p)).wait_send()
        for h in range(2):
            whole(*part(0, p, h)).wait_send()
            whole(*part(1, p, h)).wait_send()


def body(density, coords, weights, neighbours, counts):
    parts = lax.axis_size("freq")
    node_parts = lax.axis_size("node")
    times, fields, width = density.shape
    steps = times * parts
    assert times == 16 and fields == parts and width == WIDTH
    rows = times * fields
    hbm = pl.BlockSpec(memory_space=pltpu.HBM)
    buffer = pltpu.VMEM((PATCH_DEV, steps, PATCH), jnp.float32)
    half_buffer = pltpu.VMEM((PATCH_DEV, 2, steps // 2, PATCH), jnp.float32)
    pairs = PATCH_DEV * NEAR_MOST * PATCH
    operands = [
        density.reshape(rows, width),
        jnp.asarray(transform_tables(steps)),
        coords,
        weights.reshape(1, width),
        neighbours,
        counts,
        jnp.asarray(laplace_table(steps)),
    ]
    operands = [pltpu.with_memory_space_constraint(operand, pltpu.HBM) for operand in operands]
    result = pl.pallas_call(
        functools.partial(kernel, parts, node_parts),
        out_shape=jax.ShapeDtypeStruct((PATCH_DEV, rows, PATCH), jnp.float32),
        in_specs=[hbm] * len(operands),
        out_specs=pl.BlockSpec(memory_space=pltpu.VMEM),
        scratch_shapes=[
            pltpu.VMEM((PATCH_DEV, rows, PATCH), jnp.float32),
            pltpu.VMEM((4 * steps, steps), jnp.bfloat16),
            pltpu.VMEM((3, width), jnp.float32),
            pltpu.VMEM((1, width), jnp.float32),
            pltpu.SMEM((PATCH_DEV, NEAR_MOST), jnp.int32),
            pltpu.SMEM((PATCH_DEV,), jnp.int32),
            pltpu.SMEM((2, steps // 2), jnp.float32),
            buffer,
            buffer,
            half_buffer,
            pltpu.VMEM((3 * PATCH_DEV, steps // 2, PATCH), jnp.float32),
            pltpu.VMEM((3 * PATCH_DEV, steps // 2, PATCH), jnp.float32),
            pltpu.VMEM((2, PATCH_DEV * NEAR_MOST, steps // 2, PATCH), jnp.float32),
            half_buffer,
            half_buffer,
            buffer,
            buffer,
            pltpu.VMEM((3 * PATCH_DEV, 8, PATCH), jnp.float32),
            pltpu.VMEM((pairs, PATCH), jnp.float32),
            pltpu.VMEM((pairs, PATCH), jnp.float32),
            pltpu.VMEM((8 * pairs, 2 * PATCH), jnp.bfloat16),
            pltpu.VMEM((8 * pairs, 2 * PATCH), jnp.bfloat16),
            pltpu.SemaphoreType.DMA((8,)),
            pltpu.SemaphoreType.REGULAR,
            pltpu.SemaphoreType.DMA((2, PATCH_DEV)),
            pltpu.SemaphoreType.DMA((2, PATCH_DEV)),
            pltpu.SemaphoreType.DMA((2, PATCH_DEV, 2)),
            pltpu.SemaphoreType.DMA((2, PATCH_DEV, 2)),
            pltpu.SemaphoreType.DMA((2, PATCH_DEV, 2)),
            pltpu.SemaphoreType.DMA((2, PATCH_DEV, 2)),
            pltpu.SemaphoreType.DMA((2,)),
            pltpu.SemaphoreType.DMA((2,)),
        ],
        compiler_params=pltpu.CompilerParams(
            collective_id=0, has_side_effects=True, vmem_limit_bytes=40_000_000
        ),
    )(*operands)
    return jnp.swapaxes(result.reshape(PATCH_DEV, times, fields, PATCH), 0, 1).swapaxes(1, 2).reshape(times, fields, width)


def solution(mesh):
    placed = (P("freq", None, "node"), P(None, "node"), P("node"), P("node", None), P("node"))
    return jax.shard_map(
        body, mesh=mesh, in_specs=placed, out_specs=P("freq", None, "node"), check_vma=False
    )
```

```python
import functools
import math

import jax
import jax.numpy as jnp
import ml_dtypes
import numpy as np
from jax import lax
from jax.experimental import pallas as pl
from jax.experimental.pallas import tpu as pltpu
from jax.sharding import PartitionSpec as P

MESH = pl.DeviceIdType.MESH
PATCH = 128
PATCH_DEV = 2
NEAR_MOST = 4
OFFSETS = 5
WIDTH = PATCH * PATCH_DEV
DECAY = 0.1
SMOOTH = 0.25
GEN_ROWS = 64


def split_bf16(table):
    high = table.astype(np.float32).astype(ml_dtypes.bfloat16)
    low = (table - high.astype(np.float64)).astype(np.float32).astype(ml_dtypes.bfloat16)
    return high, low


def transform_tables(steps):
    freq = np.arange(steps // 2)[:, None, None]
    part = np.arange(2)[None, :, None]
    time = np.arange(steps)[None, None, :]
    angle = ((2 * freq + 1) * time % (2 * steps)) * (np.pi / steps)
    waves = np.where(part == 0, np.cos(angle), np.sin(angle)).reshape(steps, steps)
    growth = DECAY ** (np.arange(steps) / steps)
    forward = waves * growth[None, :]
    inverse = waves.T * (2.0 / steps / growth)[:, None]
    return np.concatenate(split_bf16(forward) + split_bf16(inverse), axis=0)


def laplace_table(steps):
    angle = (2 * np.arange(steps // 2) + 1) * (np.pi / steps)
    zeta = DECAY ** (1.0 / steps) * np.exp(1j * angle)
    delta = (1 - zeta) + (1 - zeta) ** 2 / 2
    return np.stack([-delta.real * np.log2(np.e), delta.imag / (2 * np.pi)]).astype(np.float32)


def fit_even(function, degree):
    nodes = 0.125 + 0.125 * np.cos(np.pi * (np.arange(200) + 0.5) / 200)
    fitted = np.polynomial.chebyshev.Chebyshev.fit(nodes, function(np.sqrt(nodes)), degree, domain=[0, 0.25])
    return [float(c) for c in fitted.convert(kind=np.polynomial.Polynomial).coef]


SINE = fit_even(lambda f: np.sin(np.pi * f) / f, 4)
COSINE = fit_even(lambda f: np.cos(np.pi * f), 4)


def horner(coefficients, value):
    total = coefficients[-1] * value + coefficients[-2]
    for coefficient in coefficients[-3::-1]:
        total = total * value + coefficient
    return total


def halves(value):
    high = value.astype(jnp.bfloat16)
    return high, (value - high.astype(jnp.float32)).astype(jnp.bfloat16)


def dot(left, right):
    return jnp.dot(left, right, preferred_element_type=jnp.float32)


def kernel(
    parts,
    x_hbm,
    table_hbm,
    coords_hbm,
    weights_hbm,
    near_hbm,
    counts_hbm,
    laplace_hbm,
    out_ref,
    x_vmem,
    table,
    coords_ref,
    weights_ref,
    near_ref,
    counts_ref,
    laplace_ref,
    send1,
    relay,
    recv1,
    send2,
    halo,
    send3,
    recv3,
    send4,
    recv4,
    place_own,
    places,
    distance,
    static,
    kern_high,
    kern_low,
    local_sem,
    chain_sem,
    relay_send,
    relay_recv,
    send_sem,
    recv_sem,
    share_recv,
    halo_send,
    halo_recv,
    spread_send,
    spread_recv,
    place_send,
    place_recv,
):
    z = lax.axis_index("freq")
    node = lax.axis_index("node")
    core = lax.rem(node, 2)
    column = node // 2
    side = math.isqrt(parts)
    steps = parts * 16
    fields = parts
    reach = parts // 4
    total_patches = 2 * parts * PATCH_DEV
    diagonal = z == column

    def shifted(k):
        return lax.rem(z + k, parts)

    def moved(dy, dx):
        return lax.rem(column // side + dy, side) * side + lax.rem(lax.rem(column, side) + dx, side)

    def hops(k, count):
        return min(k, count - k)

    planar = [(dy, dx) for dy in range(side) for dx in range(side) if dy or dx]
    planar.sort(key=lambda move: hops(move[0], side) + hops(move[1], side))
    near_first = [moved(dy, dx) for dy, dx in planar]
    far_first = near_first[::-1]
    along = sorted(range(1, parts), key=lambda k: -hops(k, parts))
    right = {"node": node + 1 - 2 * core, "freq": lax.rem(z + core, parts)}
    left = {"node": node + 1 - 2 * core, "freq": lax.rem(z + parts - 1 + core, parts)}

    barrier = pltpu.get_barrier_semaphore()
    greeted = [{"freq": shifted(k)} for k in along if hops(k, parts) <= reach]
    greeted += [{"node": 2 * other + core} for other in near_first] + [left, right]
    for device in greeted:
        pl.semaphore_signal(barrier, inc=1, device_id=device, device_id_type=MESH)

    loads = [
        pltpu.make_async_copy(x_hbm.at[:, pl.ds(p * PATCH, PATCH)], x_vmem.at[p], local_sem.at[p])
        for p in range(PATCH_DEV)
    ]
    for source, target in (
        (coords_hbm, coords_ref),
        (weights_hbm, weights_ref),
        (near_hbm, near_ref),
        (counts_hbm, counts_ref),
        (laplace_hbm, laplace_ref),
        (table_hbm, table),
    ):
        loads.append(pltpu.make_async_copy(source, target, local_sem.at[len(loads)]))
    for load in loads:
        load.start()

    def block(index):
        return pl.ds(pl.multiple_of(index * 16, 16), 16)

    for p in range(PATCH_DEV):
        loads[p].wait()
        for f in range(fields):
            send1[p, pl.ds(f * 16, 16), :] = x_vmem[p, pl.ds(f, 16, stride=fields), :]
        relay[p, block(column), :] = send1[p, block(column), :]
    for load in loads[2:7]:
        load.wait()
    lanes = lax.broadcasted_iota(jnp.int32, (8, PATCH), 1)
    masks = jnp.zeros((8, PATCH), jnp.float32)
    for p in range(PATCH_DEV):
        span = pl.ds(p * PATCH, PATCH)
        place_own[4 * p : 4 * p + 3, :] = coords_ref[:, span]
        place_own[4 * p + 3 : 4 * p + 4, :] = weights_ref[:, span]
        for o in range(OFFSETS):
            wanted = lax.rem(node * PATCH_DEV + p + o - OFFSETS // 2 + total_patches, total_patches)
            mask = jnp.float32(0)
            for k in range(NEAR_MOST):
                used = jnp.logical_and(near_ref[p, k] == wanted, k < counts_ref[p])
                mask = mask + jnp.where(used, 1.0, 0.0)
            masks = jnp.where(lanes == p * OFFSETS + o, mask, masks)
    place_own[8:16, :] = masks
    pl.semaphore_wait(barrier, len(greeted))

    def push(device, source, target, sends, receives):
        pltpu.make_async_remote_copy(
            src_ref=source,
            dst_ref=target,
            send_sem=sends,
            recv_sem=receives,
            device_id=device,
            device_id_type=MESH,
        ).start()

    def pending(source, target, count, sends, receives):
        span = pl.ds(0, count * 16)
        return pltpu.make_async_remote_copy(
            src_ref=source.at[span],
            dst_ref=target.at[span],
            send_sem=sends,
            recv_sem=receives,
            device_id=right,
            device_id_type=MESH,
        )

    def stage(index, p):
        source, target = (
            (relay.at[p], recv1.at[p]),
            (send2.at[p], halo.at[2 + p]),
            (send3.at[p], recv3.at[p]),
            (send4.at[p], recv4.at[p]),
        )[index]
        return source, target, send_sem.at[index, p], recv_sem.at[index, p]

    def rest(index, p, count):
        source, target, sends, receives = stage(index, p)
        return pending(source, target, count, sends, receives)

    for k in (reach, parts - reach):
        pl.semaphore_signal(chain_sem, inc=1, device_id={"freq": shifted(k)}, device_id_type=MESH)
    def place_copy(index):
        return pltpu.make_async_remote_copy(
            src_ref=place_own,
            dst_ref=places.at[1],
            send_sem=spread_send.at[index],
            recv_sem=spread_recv,
            device_id={"node": 2 * near_first[index] + core},
            device_id_type=MESH,
        )

    @pl.when(diagonal)
    def _():
        for index in range(parts - 1):
            place_copy(index).start()
        places[1] = place_own[...]

    for p in range(PATCH_DEV):
        for other in near_first:
            push(
                {"node": 2 * other + core},
                send1.at[p, block(other)],
                relay.at[p, block(column)],
                relay_send.at[p],
                relay_recv.at[p, column],
            )

    pl.semaphore_wait(chain_sem, 2)

    def forward(p, source):
        _, _, sends, receives = stage(0, p)
        push({"freq": source}, relay.at[p, block(source)], recv1.at[p, block(z)], sends, receives)

    def keep(p):
        @pl.when(jnp.logical_not(diagonal))
        def _():
            arrived(p, z)

        recv1[p, block(z), :] = relay[p, block(z), :]

    def arrived(p, source):
        pltpu.make_async_remote_copy(
            src_ref=relay.at[p, block(source)],
            dst_ref=relay.at[p, block(source)],
            send_sem=relay_send.at[p],
            recv_sem=relay_recv.at[p, source],
            device_id=right,
            device_id_type=MESH,
        ).wait_recv()

    def forward_as_arrived(p):
        @pl.when(jnp.logical_not(diagonal))
        def _():
            forward(p, column)

        for other in near_first:

            @pl.when(other != z)
            def _(other=other):
                arrived(p, other)
                forward(p, other)

    def forward_far_first(p):
        for k in along:
            source = shifted(k)

            @pl.when(source != column)
            def _(source=source):
                arrived(p, source)

            forward(p, source)

    forward_as_arrived(0)

    @pl.when(jnp.logical_not(diagonal))
    def _():
        place_copy(0).wait_recv()

    place_copies = [
        pltpu.make_async_remote_copy(
            src_ref=places.at[1],
            dst_ref=places.at[slot],
            send_sem=place_send.at[slot // 2],
            recv_sem=place_recv.at[slot // 2],
            device_id=device,
            device_id_type=MESH,
        )
        for device, slot in ((right, 0), (left, 2))
    ]
    for copy in place_copies:
        copy.start()
    forward_far_first(1)
    for p in range(PATCH_DEV):
        keep(p)
    for copy in place_copies:
        copy.wait_recv()

    turned = [places[index].T for index in range(3)]
    for p in range(PATCH_DEV):
        for o in range(OFFSETS):
            other = turned[(p + o) // PATCH_DEV]
            first = 4 * ((p + o) % PATCH_DEV)
            total = SMOOTH
            for c in range(3):
                apart = other[:, first + c : first + c + 1] - places[1, 4 * p + c : 4 * p + c + 1, :]
                total = total + apart * apart
            inverse = lax.rsqrt(total)
            lane = p * OFFSETS + o
            scale = places[1, 8:9, lane : lane + 1] * (1.0 / (4.0 * np.pi))
            rows = pl.ds((p * OFFSETS + o) * PATCH, PATCH)
            distance[rows, :] = total * inverse
            static[rows, :] = (other[:, first + 3 : first + 4] * scale) * inverse

    blocks = PATCH_DEV * OFFSETS * PATCH // GEN_ROWS

    def generate(step, carry):
        l = step // blocks
        rows = pl.ds(pl.multiple_of(step % blocks * GEN_ROWS, GEN_ROWS), GEN_ROWS)
        radius = distance[rows, :]
        decaying = jnp.exp2(radius * laplace_ref[0, column * 8 + l]) * static[rows, :]
        turns = radius * laplace_ref[1, column * 8 + l]
        turns = turns - jnp.round(turns)
        square = turns * turns
        sine = horner(SINE, square) * turns
        cosine = horner([-c for c in COSINE], square)
        double = decaying * sine
        double = double + double
        real_high, real_low = halves(decaying - double * sine)
        imag_high, imag_low = halves(double * cosine)
        into = pl.ds(pl.multiple_of(step * GEN_ROWS, GEN_ROWS), GEN_ROWS)
        kern_high[into, 0:PATCH] = real_high
        kern_high[into, PATCH : 2 * PATCH] = imag_high
        kern_low[into, 0:PATCH] = real_low
        kern_low[into, PATCH : 2 * PATCH] = imag_low
        return carry

    lax.fori_loop(0, 4 * blocks, generate, 0)

    def transform(index, data):
        data_high, data_low = halves(data)
        table_high = table[pl.ds(2 * index * steps, steps), :]
        table_low = table[pl.ds((2 * index + 1) * steps, steps), :]
        first = dot(table_high, jnp.concatenate([data_high, data_low], axis=1))
        return first[:, :PATCH] + first[:, PATCH:] + dot(table_low, data_high)

    def across(index, p, receives=None):
        source, target, sends, arrivals = stage(index, p)
        receives = arrivals if receives is None else receives
        for other in far_first:
            push({"node": 2 * other + core}, source.at[block(other)], target.at[block(column)], sends, receives)

    def forward_transform(p, receives=None):
        rest(0, p, parts - 1).wait_recv()
        send2[p] = transform(0, recv1[p])
        halo[2 + p, block(column), :] = send2[p, block(column), :]
        across(1, p, receives)

    sides = ((right, 0), (left, 4))

    def halo_copy(p, slot, device):
        return pltpu.make_async_remote_copy(
            src_ref=halo.at[2 + p],
            dst_ref=halo.at[slot + p],
            send_sem=halo_send.at[slot // 4, p],
            recv_sem=halo_recv.at[slot // 4, p],
            device_id=device,
            device_id_type=MESH,
        )

    halo_copies = [halo_copy(p, slot, device) for p in range(PATCH_DEV) for device, slot in sides]

    def share_chunk(p, index):
        for device, slot in sides:
            push(
                device,
                halo.at[2 + p, block(index)],
                halo.at[slot + p, block(index)],
                halo_send.at[slot // 4, p],
                halo_recv.at[slot // 4, p],
            )

    loads[7].wait()
    forward_transform(0)
    forward_transform(1, share_recv.at[column])
    share_chunk(1, column)
    lax.fori_loop(4 * blocks, 6 * blocks, generate, 0)
    rest(1, 0, parts - 1).wait_recv()
    for copy in halo_copies[:2]:
        copy.start()
    for other in near_first:
        pltpu.make_async_remote_copy(
            src_ref=halo.at[3, block(other)],
            dst_ref=halo.at[3, block(other)],
            send_sem=send_sem.at[1, 1],
            recv_sem=share_recv.at[other],
            device_id=right,
            device_id_type=MESH,
        ).wait_recv()
        share_chunk(1, other)
    lax.fori_loop(6 * blocks, 8 * blocks, generate, 0)
    for copy in halo_copies:
        copy.wait_recv()

    for p in range(PATCH_DEV):
        for l in range(8):
            both = jnp.concatenate(
                [
                    jnp.concatenate(
                        [halo[p + o, pl.ds(2 * l + ri, fields, stride=16), :] for o in range(OFFSETS)],
                        axis=1,
                    )
                    for ri in range(2)
                ],
                axis=0,
            )
            both_high, both_low = halves(both)
            rows = pl.ds((l * PATCH_DEV + p) * OFFSETS * PATCH, OFFSETS * PATCH)
            first = dot(jnp.concatenate([both_high, both_low], axis=0), kern_high[rows, :])
            total = first[: 2 * fields] + first[2 * fields :] + dot(both_high, kern_low[rows, :])
            send3[p, pl.ds(2 * l, fields, stride=16), :] = total[:fields, :PATCH] - total[fields:, PATCH:]
            send3[p, pl.ds(2 * l + 1, fields, stride=16), :] = total[fields:, :PATCH] + total[:fields, PATCH:]
        recv3[p, block(column), :] = send3[p, block(column), :]
        across(2, p)

    def home(p, k):
        source, target, sends, receives = stage(3, p)
        time = shifted(k)
        push({"node": 2 * z + core, "freq": time}, source.at[block(time)], target.at[block(column)], sends, receives)

    for p in range(PATCH_DEV):
        rest(2, p, parts - 1).wait_recv()
        send4[p] = transform(1, recv3[p])
        for k in along:
            home(p, k)

        @pl.when(diagonal)
        def _(p=p):
            recv4[p, block(column), :] = send4[p, block(column), :]

        @pl.when(jnp.logical_not(diagonal))
        def _(p=p):
            home(p, 0)

    for p in range(PATCH_DEV):

        @pl.when(diagonal)
        def _(p=p):
            rest(3, p, parts - 1).wait_recv()

        @pl.when(jnp.logical_not(diagonal))
        def _(p=p):
            rest(3, p, parts).wait_recv()

        for f in range(fields):
            out_ref[p, pl.ds(f, 16, stride=fields), :] = recv4[p, pl.ds(f * 16, 16), :]

    for copy in place_copies + halo_copies:
        copy.wait_send()
    for p in range(PATCH_DEV):
        pending(send1.at[p], relay.at[p], parts - 1, relay_send.at[p], relay_recv.at[p, 0]).wait_send()
        for index in range(3):
            rest(index, p, parts - 1).wait_send()

    @pl.when(diagonal)
    def _():
        for index in range(parts - 1):
            place_copy(index).wait_send()
        for p in range(PATCH_DEV):
            rest(3, p, parts - 1).wait_send()

    @pl.when(jnp.logical_not(diagonal))
    def _():
        for p in range(PATCH_DEV):
            rest(3, p, parts).wait_send()


def body(density, coords, weights, neighbours, counts):
    parts = lax.axis_size("freq")
    node_parts = lax.axis_size("node")
    times, fields, width = density.shape
    steps = times * parts
    assert times == 16 and fields == parts and node_parts == 2 * parts and width == WIDTH
    rows = times * fields
    hbm = pl.BlockSpec(memory_space=pltpu.HBM)
    buffer = pltpu.VMEM((PATCH_DEV, steps, PATCH), jnp.float32)
    pairs = PATCH_DEV * OFFSETS * PATCH
    operands = [
        density.reshape(rows, width),
        jnp.asarray(transform_tables(steps)),
        coords,
        weights.reshape(1, width),
        neighbours,
        counts,
        jnp.asarray(laplace_table(steps)),
    ]
    operands = [pltpu.with_memory_space_constraint(operand, pltpu.HBM) for operand in operands]
    result = pl.pallas_call(
        functools.partial(kernel, parts),
        out_shape=jax.ShapeDtypeStruct((PATCH_DEV, rows, PATCH), jnp.float32),
        in_specs=[hbm] * len(operands),
        out_specs=pl.BlockSpec(memory_space=pltpu.VMEM),
        scratch_shapes=[
            pltpu.VMEM((PATCH_DEV, rows, PATCH), jnp.float32),
            pltpu.VMEM((4 * steps, steps), jnp.bfloat16),
            pltpu.VMEM((3, width), jnp.float32),
            pltpu.VMEM((1, width), jnp.float32),
            pltpu.SMEM((PATCH_DEV, NEAR_MOST), jnp.int32),
            pltpu.SMEM((PATCH_DEV,), jnp.int32),
            pltpu.SMEM((2, steps // 2), jnp.float32),
            buffer,
            buffer,
            buffer,
            buffer,
            pltpu.VMEM((3 * PATCH_DEV, steps, PATCH), jnp.float32),
            buffer,
            buffer,
            buffer,
            buffer,
            pltpu.VMEM((16, PATCH), jnp.float32),
            pltpu.VMEM((3, 16, PATCH), jnp.float32),
            pltpu.VMEM((pairs, PATCH), jnp.float32),
            pltpu.VMEM((pairs, PATCH), jnp.float32),
            pltpu.VMEM((8 * pairs, 2 * PATCH), jnp.bfloat16),
            pltpu.VMEM((8 * pairs, 2 * PATCH), jnp.bfloat16),
            pltpu.SemaphoreType.DMA((8,)),
            pltpu.SemaphoreType.REGULAR,
            pltpu.SemaphoreType.DMA((PATCH_DEV,)),
            pltpu.SemaphoreType.DMA((PATCH_DEV, parts)),
            pltpu.SemaphoreType.DMA((4, PATCH_DEV)),
            pltpu.SemaphoreType.DMA((4, PATCH_DEV)),
            pltpu.SemaphoreType.DMA((parts,)),
            pltpu.SemaphoreType.DMA((2, PATCH_DEV)),
            pltpu.SemaphoreType.DMA((2, PATCH_DEV)),
            pltpu.SemaphoreType.DMA((parts - 1,)),
            pltpu.SemaphoreType.DMA,
            pltpu.SemaphoreType.DMA((2,)),
            pltpu.SemaphoreType.DMA((2,)),
        ],
        compiler_params=pltpu.CompilerParams(
            collective_id=0, has_side_effects=True, vmem_limit_bytes=40_000_000
        ),
    )(*operands)
    return jnp.swapaxes(result.reshape(PATCH_DEV, times, fields, PATCH), 0, 1).swapaxes(1, 2).reshape(times, fields, width)


def solution(mesh):
    placed = (P("freq", None, "node"), P(None, "node"), P("node"), P("node", None), P("node"))
    return jax.shard_map(
        body, mesh=mesh, in_specs=placed, out_specs=P("freq", None, "node"), check_vma=False
    )
```

```python
import functools
import math

import jax
import jax.numpy as jnp
import ml_dtypes
import numpy as np
from jax import lax
from jax.experimental import pallas as pl
from jax.experimental.pallas import tpu as pltpu
from jax.sharding import PartitionSpec as P

MESH = pl.DeviceIdType.MESH
PATCH = 128
PATCH_DEV = 2
NEAR_MOST = 4
OFFSETS = 5
WIDTH = PATCH * PATCH_DEV
DECAY = 0.1
SMOOTH = 0.25
GEN_ROWS = 64


def split_bf16(table):
    high = table.astype(np.float32).astype(ml_dtypes.bfloat16)
    low = (table - high.astype(np.float64)).astype(np.float32).astype(ml_dtypes.bfloat16)
    return high, low


def transform_tables(steps):
    freq = np.arange(steps // 2)[:, None, None]
    part = np.arange(2)[None, :, None]
    time = np.arange(steps)[None, None, :]
    angle = ((2 * freq + 1) * time % (2 * steps)) * (np.pi / steps)
    waves = np.where(part == 0, np.cos(angle), np.sin(angle)).reshape(steps, steps)
    growth = DECAY ** (np.arange(steps) / steps)
    forward = waves * growth[None, :]
    inverse = waves.T * (2.0 / steps / growth)[:, None]
    return np.concatenate(split_bf16(forward) + split_bf16(inverse), axis=0)


def laplace_table(steps):
    angle = (2 * np.arange(steps // 2) + 1) * (np.pi / steps)
    zeta = DECAY ** (1.0 / steps) * np.exp(1j * angle)
    delta = (1 - zeta) + (1 - zeta) ** 2 / 2
    return np.stack([-delta.real * np.log2(np.e), delta.imag / (2 * np.pi)]).astype(np.float32)


def fit_even(function, degree):
    nodes = 0.125 + 0.125 * np.cos(np.pi * (np.arange(200) + 0.5) / 200)
    fitted = np.polynomial.chebyshev.Chebyshev.fit(nodes, function(np.sqrt(nodes)), degree, domain=[0, 0.25])
    return [float(c) for c in fitted.convert(kind=np.polynomial.Polynomial).coef]


SINE = fit_even(lambda f: np.sin(np.pi * f) / f, 4)
COSINE = fit_even(lambda f: np.cos(np.pi * f), 4)


def horner(coefficients, value):
    total = coefficients[-1] * value + coefficients[-2]
    for coefficient in coefficients[-3::-1]:
        total = total * value + coefficient
    return total


def halves(value):
    high = value.astype(jnp.bfloat16)
    return high, (value - high.astype(jnp.float32)).astype(jnp.bfloat16)


def dot(left, right):
    return jnp.dot(left, right, preferred_element_type=jnp.float32)


def kernel(
    parts,
    x_hbm,
    table_hbm,
    coords_hbm,
    weights_hbm,
    near_hbm,
    counts_hbm,
    laplace_hbm,
    out_ref,
    x_vmem,
    table,
    coords_ref,
    weights_ref,
    near_ref,
    counts_ref,
    laplace_ref,
    send1,
    relay,
    recv1,
    send2,
    halo,
    send3,
    recv3,
    send4,
    recv4,
    place_own,
    places,
    distance,
    static,
    kern_high,
    kern_low,
    local_sem,
    chain_sem,
    relay_send,
    relay_recv,
    send_sem,
    recv_sem,
    halo_send,
    halo_recv,
    spread_send,
    spread_recv,
    place_send,
    place_recv,
):
    z = lax.axis_index("freq")
    node = lax.axis_index("node")
    core = lax.rem(node, 2)
    column = node // 2
    side = math.isqrt(parts)
    steps = parts * 16
    fields = parts
    reach = parts // 4
    total_patches = 2 * parts * PATCH_DEV
    diagonal = z == column

    def shifted(k):
        return lax.rem(z + k, parts)

    def moved(dy, dx):
        return lax.rem(column // side + dy, side) * side + lax.rem(lax.rem(column, side) + dx, side)

    def hops(k, count):
        return min(k, count - k)

    planar = [(dy, dx) for dy in range(side) for dx in range(side) if dy or dx]
    planar.sort(key=lambda move: hops(move[0], side) + hops(move[1], side))
    near_first = [moved(dy, dx) for dy, dx in planar]
    far_first = near_first[::-1]
    along = sorted(range(1, parts), key=lambda k: -hops(k, parts))
    right = {"node": node + 1 - 2 * core, "freq": lax.rem(z + core, parts)}
    left = {"node": node + 1 - 2 * core, "freq": lax.rem(z + parts - 1 + core, parts)}

    barrier = pltpu.get_barrier_semaphore()
    greeted = [{"freq": shifted(k)} for k in along if hops(k, parts) <= reach]
    greeted += [{"node": 2 * other + core} for other in near_first] + [left, right]
    for device in greeted:
        pl.semaphore_signal(barrier, inc=1, device_id=device, device_id_type=MESH)

    loads = [
        pltpu.make_async_copy(x_hbm.at[:, pl.ds(p * PATCH, PATCH)], x_vmem.at[p], local_sem.at[p])
        for p in range(PATCH_DEV)
    ]
    for source, target in (
        (coords_hbm, coords_ref),
        (weights_hbm, weights_ref),
        (near_hbm, near_ref),
        (counts_hbm, counts_ref),
        (laplace_hbm, laplace_ref),
        (table_hbm, table),
    ):
        loads.append(pltpu.make_async_copy(source, target, local_sem.at[len(loads)]))
    for load in loads:
        load.start()

    def block(index):
        return pl.ds(pl.multiple_of(index * 16, 16), 16)

    for p in range(PATCH_DEV):
        loads[p].wait()
        for f in range(fields):
            send1[p, pl.ds(f * 16, 16), :] = x_vmem[p, pl.ds(f, 16, stride=fields), :]
        relay[p, block(column), :] = send1[p, block(column), :]
    for load in loads[2:7]:
        load.wait()
    lanes = lax.broadcasted_iota(jnp.int32, (8, PATCH), 1)
    masks = jnp.zeros((8, PATCH), jnp.float32)
    for p in range(PATCH_DEV):
        span = pl.ds(p * PATCH, PATCH)
        place_own[4 * p : 4 * p + 3, :] = coords_ref[:, span]
        place_own[4 * p + 3 : 4 * p + 4, :] = weights_ref[:, span]
        for o in range(OFFSETS):
            wanted = lax.rem(node * PATCH_DEV + p + o - OFFSETS // 2 + total_patches, total_patches)
            mask = jnp.float32(0)
            for k in range(NEAR_MOST):
                used = jnp.logical_and(near_ref[p, k] == wanted, k < counts_ref[p])
                mask = mask + jnp.where(used, 1.0, 0.0)
            masks = jnp.where(lanes == p * OFFSETS + o, mask, masks)
    place_own[8:16, :] = masks
    pl.semaphore_wait(barrier, len(greeted))

    def push(device, source, target, sends, receives):
        pltpu.make_async_remote_copy(
            src_ref=source,
            dst_ref=target,
            send_sem=sends,
            recv_sem=receives,
            device_id=device,
            device_id_type=MESH,
        ).start()

    def pending(source, target, count, sends, receives):
        span = pl.ds(0, count * 16)
        return pltpu.make_async_remote_copy(
            src_ref=source.at[span],
            dst_ref=target.at[span],
            send_sem=sends,
            recv_sem=receives,
            device_id=right,
            device_id_type=MESH,
        )

    def stage(index, p):
        source, target = (
            (relay.at[p], recv1.at[p]),
            (send2.at[p], halo.at[2 + p]),
            (send3.at[p], recv3.at[p]),
            (send4.at[p], recv4.at[p]),
        )[index]
        return source, target, send_sem.at[index, p], recv_sem.at[index, p]

    def rest(index, p, count):
        source, target, sends, receives = stage(index, p)
        return pending(source, target, count, sends, receives)

    for k in (reach, parts - reach):
        pl.semaphore_signal(chain_sem, inc=1, device_id={"freq": shifted(k)}, device_id_type=MESH)
    def place_copy(index):
        return pltpu.make_async_remote_copy(
            src_ref=place_own,
            dst_ref=places.at[1],
            send_sem=spread_send.at[index],
            recv_sem=spread_recv,
            device_id={"node": 2 * near_first[index] + core},
            device_id_type=MESH,
        )

    @pl.when(diagonal)
    def _():
        for index in range(parts - 1):
            place_copy(index).start()
        places[1] = place_own[...]

    for p in range(PATCH_DEV):
        for other in far_first:
            push(
                {"node": 2 * other + core},
                send1.at[p, block(other)],
                relay.at[p, block(column)],
                relay_send.at[p],
                relay_recv.at[p, column],
            )

    pl.semaphore_wait(chain_sem, 2)

    def forward(p, source):
        _, _, sends, receives = stage(0, p)
        push({"freq": source}, relay.at[p, block(source)], recv1.at[p, block(z)], sends, receives)

    def keep(p):
        @pl.when(jnp.logical_not(diagonal))
        def _():
            arrived(p, z)

        recv1[p, block(z), :] = relay[p, block(z), :]

    def arrived(p, source):
        pltpu.make_async_remote_copy(
            src_ref=relay.at[p, block(source)],
            dst_ref=relay.at[p, block(source)],
            send_sem=relay_send.at[p],
            recv_sem=relay_recv.at[p, source],
            device_id=right,
            device_id_type=MESH,
        ).wait_recv()

    def forward_as_arrived(p):
        @pl.when(jnp.logical_not(diagonal))
        def _():
            forward(p, column)

        for other in near_first:

            @pl.when(other != z)
            def _(other=other):
                arrived(p, other)
                forward(p, other)

    def forward_far_first(p):
        for k in along:
            source = shifted(k)

            @pl.when(source != column)
            def _(source=source):
                arrived(p, source)

            forward(p, source)

    forward_as_arrived(0)

    @pl.when(jnp.logical_not(diagonal))
    def _():
        place_copy(0).wait_recv()

    place_copies = [
        pltpu.make_async_remote_copy(
            src_ref=places.at[1],
            dst_ref=places.at[slot],
            send_sem=place_send.at[slot // 2],
            recv_sem=place_recv.at[slot // 2],
            device_id=device,
            device_id_type=MESH,
        )
        for device, slot in ((right, 0), (left, 2))
    ]
    for copy in place_copies:
        copy.start()
    forward_far_first(1)
    for p in range(PATCH_DEV):
        keep(p)
    for copy in place_copies:
        copy.wait_recv()

    turned = [places[index].T for index in range(3)]
    for p in range(PATCH_DEV):
        for o in range(OFFSETS):
            other = turned[(p + o) // PATCH_DEV]
            first = 4 * ((p + o) % PATCH_DEV)
            total = SMOOTH
            for c in range(3):
                apart = other[:, first + c : first + c + 1] - places[1, 4 * p + c : 4 * p + c + 1, :]
                total = total + apart * apart
            inverse = lax.rsqrt(total)
            lane = p * OFFSETS + o
            scale = places[1, 8:9, lane : lane + 1] * (1.0 / (4.0 * np.pi))
            rows = pl.ds((p * OFFSETS + o) * PATCH, PATCH)
            distance[rows, :] = total * inverse
            static[rows, :] = (other[:, first + 3 : first + 4] * scale) * inverse

    blocks = PATCH_DEV * OFFSETS * PATCH // GEN_ROWS

    def generate(step, carry):
        l = step // blocks
        rows = pl.ds(pl.multiple_of(step % blocks * GEN_ROWS, GEN_ROWS), GEN_ROWS)
        radius = distance[rows, :]
        decaying = jnp.exp2(radius * laplace_ref[0, column * 8 + l]) * static[rows, :]
        turns = radius * laplace_ref[1, column * 8 + l]
        turns = turns - jnp.round(turns)
        square = turns * turns
        sine = horner(SINE, square) * turns
        cosine = horner([-c for c in COSINE], square)
        double = decaying * sine
        double = double + double
        real_high, real_low = halves(decaying - double * sine)
        imag_high, imag_low = halves(double * cosine)
        into = pl.ds(pl.multiple_of(step * GEN_ROWS, GEN_ROWS), GEN_ROWS)
        kern_high[into, 0:PATCH] = real_high
        kern_high[into, PATCH : 2 * PATCH] = imag_high
        kern_low[into, 0:PATCH] = real_low
        kern_low[into, PATCH : 2 * PATCH] = imag_low
        return carry

    lax.fori_loop(0, 6 * blocks, generate, 0)

    def transform(index, data):
        data_high, data_low = halves(data)
        table_high = table[pl.ds(2 * index * steps, steps), :]
        table_low = table[pl.ds((2 * index + 1) * steps, steps), :]
        first = dot(table_high, jnp.concatenate([data_high, data_low], axis=1))
        return first[:, :PATCH] + first[:, PATCH:] + dot(table_low, data_high)

    def across(index, p):
        source, target, sends, receives = stage(index, p)
        for other in far_first:
            push({"node": 2 * other + core}, source.at[block(other)], target.at[block(column)], sends, receives)

    def forward_transform(p):
        rest(0, p, parts - 1).wait_recv()
        send2[p] = transform(0, recv1[p])
        halo[2 + p, block(column), :] = send2[p, block(column), :]
        across(1, p)

    sides = ((right, 0), (left, 4))

    def halo_copy(p, slot, device):
        return pltpu.make_async_remote_copy(
            src_ref=halo.at[2 + p],
            dst_ref=halo.at[slot + p],
            send_sem=halo_send.at[slot // 4, p],
            recv_sem=halo_recv.at[slot // 4, p],
            device_id=device,
            device_id_type=MESH,
        )

    halo_copies = [halo_copy(p, slot, device) for p in range(PATCH_DEV) for device, slot in sides]

    loads[7].wait()
    for p in range(PATCH_DEV):
        forward_transform(p)
    lax.fori_loop(6 * blocks, 8 * blocks, generate, 0)
    for p in range(PATCH_DEV):
        rest(1, p, parts - 1).wait_recv()
        for copy in halo_copies[2 * p : 2 * p + 2]:
            copy.start()
    for copy in halo_copies:
        copy.wait_recv()

    for p in range(PATCH_DEV):
        for l in range(8):
            both = jnp.concatenate(
                [
                    jnp.concatenate(
                        [halo[p + o, pl.ds(2 * l + ri, fields, stride=16), :] for o in range(OFFSETS)],
                        axis=1,
                    )
                    for ri in range(2)
                ],
                axis=0,
            )
            both_high, both_low = halves(both)
            rows = pl.ds((l * PATCH_DEV + p) * OFFSETS * PATCH, OFFSETS * PATCH)
            first = dot(jnp.concatenate([both_high, both_low], axis=0), kern_high[rows, :])
            total = first[: 2 * fields] + first[2 * fields :] + dot(both_high, kern_low[rows, :])
            send3[p, pl.ds(2 * l, fields, stride=16), :] = total[:fields, :PATCH] - total[fields:, PATCH:]
            send3[p, pl.ds(2 * l + 1, fields, stride=16), :] = total[fields:, :PATCH] + total[:fields, PATCH:]
        recv3[p, block(column), :] = send3[p, block(column), :]
        across(2, p)

    def home(p, k):
        source, target, sends, receives = stage(3, p)
        time = shifted(k)
        push({"node": 2 * z + core, "freq": time}, source.at[block(time)], target.at[block(column)], sends, receives)

    for p in range(PATCH_DEV):
        rest(2, p, parts - 1).wait_recv()
        send4[p] = transform(1, recv3[p])
        for k in along:
            home(p, k)

        @pl.when(diagonal)
        def _(p=p):
            recv4[p, block(column), :] = send4[p, block(column), :]

        @pl.when(jnp.logical_not(diagonal))
        def _(p=p):
            home(p, 0)

    for p in range(PATCH_DEV):

        @pl.when(diagonal)
        def _(p=p):
            rest(3, p, parts - 1).wait_recv()

        @pl.when(jnp.logical_not(diagonal))
        def _(p=p):
            rest(3, p, parts).wait_recv()

        for f in range(fields):
            out_ref[p, pl.ds(f, 16, stride=fields), :] = recv4[p, pl.ds(f * 16, 16), :]

    for copy in place_copies + halo_copies:
        copy.wait_send()
    for p in range(PATCH_DEV):
        pending(send1.at[p], relay.at[p], parts - 1, relay_send.at[p], relay_recv.at[p, 0]).wait_send()
        for index in range(3):
            rest(index, p, parts - 1).wait_send()

    @pl.when(diagonal)
    def _():
        for index in range(parts - 1):
            place_copy(index).wait_send()
        for p in range(PATCH_DEV):
            rest(3, p, parts - 1).wait_send()

    @pl.when(jnp.logical_not(diagonal))
    def _():
        for p in range(PATCH_DEV):
            rest(3, p, parts).wait_send()


def body(density, coords, weights, neighbours, counts):
    parts = lax.axis_size("freq")
    node_parts = lax.axis_size("node")
    times, fields, width = density.shape
    steps = times * parts
    assert times == 16 and fields == parts and node_parts == 2 * parts and width == WIDTH
    rows = times * fields
    hbm = pl.BlockSpec(memory_space=pltpu.HBM)
    buffer = pltpu.VMEM((PATCH_DEV, steps, PATCH), jnp.float32)
    pairs = PATCH_DEV * OFFSETS * PATCH
    operands = [
        density.reshape(rows, width),
        jnp.asarray(transform_tables(steps)),
        coords,
        weights.reshape(1, width),
        neighbours,
        counts,
        jnp.asarray(laplace_table(steps)),
    ]
    operands = [pltpu.with_memory_space_constraint(operand, pltpu.HBM) for operand in operands]
    result = pl.pallas_call(
        functools.partial(kernel, parts),
        out_shape=jax.ShapeDtypeStruct((PATCH_DEV, rows, PATCH), jnp.float32),
        in_specs=[hbm] * len(operands),
        out_specs=pl.BlockSpec(memory_space=pltpu.VMEM),
        scratch_shapes=[
            pltpu.VMEM((PATCH_DEV, rows, PATCH), jnp.float32),
            pltpu.VMEM((4 * steps, steps), jnp.bfloat16),
            pltpu.VMEM((3, width), jnp.float32),
            pltpu.VMEM((1, width), jnp.float32),
            pltpu.SMEM((PATCH_DEV, NEAR_MOST), jnp.int32),
            pltpu.SMEM((PATCH_DEV,), jnp.int32),
            pltpu.SMEM((2, steps // 2), jnp.float32),
            buffer,
            buffer,
            buffer,
            buffer,
            pltpu.VMEM((3 * PATCH_DEV, steps, PATCH), jnp.float32),
            buffer,
            buffer,
            buffer,
            buffer,
            pltpu.VMEM((16, PATCH), jnp.float32),
            pltpu.VMEM((3, 16, PATCH), jnp.float32),
            pltpu.VMEM((pairs, PATCH), jnp.float32),
            pltpu.VMEM((pairs, PATCH), jnp.float32),
            pltpu.VMEM((8 * pairs, 2 * PATCH), jnp.bfloat16),
            pltpu.VMEM((8 * pairs, 2 * PATCH), jnp.bfloat16),
            pltpu.SemaphoreType.DMA((8,)),
            pltpu.SemaphoreType.REGULAR,
            pltpu.SemaphoreType.DMA((PATCH_DEV,)),
            pltpu.SemaphoreType.DMA((PATCH_DEV, parts)),
            pltpu.SemaphoreType.DMA((4, PATCH_DEV)),
            pltpu.SemaphoreType.DMA((4, PATCH_DEV)),
            pltpu.SemaphoreType.DMA((2, PATCH_DEV)),
            pltpu.SemaphoreType.DMA((2, PATCH_DEV)),
            pltpu.SemaphoreType.DMA((parts - 1,)),
            pltpu.SemaphoreType.DMA,
            pltpu.SemaphoreType.DMA((2,)),
            pltpu.SemaphoreType.DMA((2,)),
        ],
        compiler_params=pltpu.CompilerParams(
            collective_id=0, has_side_effects=True, vmem_limit_bytes=40_000_000
        ),
    )(*operands)
    return jnp.swapaxes(result.reshape(PATCH_DEV, times, fields, PATCH), 0, 1).swapaxes(1, 2).reshape(times, fields, width)


def solution(mesh):
    placed = (P("freq", None, "node"), P(None, "node"), P("node"), P("node", None), P("node"))
    return jax.shard_map(
        body, mesh=mesh, in_specs=placed, out_specs=P("freq", None, "node"), check_vma=False
    )
```
